32 devices in a mesh: section: 4 (over y, core), expert: 8 (over z, x).
Axes of the slice: x: 2, y: 2, z: 4, core: 2. Of those that a mesh axis runs over, the one named last changes fastest.
Arguments:
- inputs: bfloat16 [4, 1024, 1024], P('section', 'expert'), may hold values from -6 to 6
- out_grads: bfloat16 [4, 1024, 1024], P('section', 'expert'), may hold values from -6 to 6
- expert_ids: int32 [4, 1024, 8], P('section', 'expert'), may hold values from 0 to 15, all different within a row; in each aligned block of 128 rows (0 to 127, 128 to 255, ..., all dimensions but the last counted through in order) at most 96 rows name the same one
- route_levels: int32 [4, 1024, 8], P('section', 'expert'), may hold values from 8 to 256
- w_gate: bfloat16 [4, 16, 1024, 384], P('section', 'expert'), may hold values from -0.1875 to 0.1875
- w_up: bfloat16 [4, 16, 1024, 384], P('section', 'expert'), may hold values from -0.1875 to 0.1875
- w_down: bfloat16 [4, 16, 384, 1024], P('section', 'expert'), may hold values from -0.3125 to 0.3125
Outputs:
- upstream: bfloat16 [4, 1024, 1024], P('section', 'expert')
- route_grad: bfloat16 [4, 1024, 8], P('section', 'expert')
- gate_update: bfloat16 [4, 16, 1024, 384], P('section', 'expert')
- up_update: bfloat16 [4, 16, 1024, 384], P('section', 'expert')
- down_update: bfloat16 [4, 16, 384, 1024], P('section', 'expert')
The draws below stay inside these ranges and needn't reach their ends.
Inputs may be any that keep to these rules, and one draw needn't show every extreme that they name: `expert_ids`: each token names 8 different experts; among the 128 tokens of one aligned block no expert is named more than 96 times.
All inputs are finite; a program needn't handle non-finite values.
Results may differ from the reference program's by a relative error of at most 0.0064.
Values may be sent and summed in bfloat16 or wider, within the bound.
A program may use at most 128 MiB of HBM per device.

```python
import math
import jax
import jax.numpy as jnp
import numpy as np
from jax import lax

D = 1024
H = 384
TOPK = 8
TOK_DEV = 128
EXPERTS = 16
CAP = 96
SECTIONS = 4
TOKENS = 1024
N_EXPERT = 8


def set_ends(entries, own_key, least, high):
    shape = entries.shape
    index_at = [jax.random.randint(jax.random.fold_in(own_key, axis), (), 0, shape[axis]) for axis in range(len(shape))]
    entries = entries.at[tuple(index_at)].set(least)
    longest = shape.index(max(shape))
    index_at[longest] = (index_at[longest] + 1) % shape[longest]
    return entries.at[tuple(index_at)].set(high)


def block_scale(key, extent, split, least, high):
    factor_of = 1.0
    for position, blocks in split:
        heights = jax.random.uniform(jax.random.fold_in(jax.random.fold_in(key, 6), position), (blocks,), jnp.float32, least / len(split), high / len(split))
        factor_of = factor_of * jnp.repeat(jnp.exp(heights), extent[position] // blocks).reshape((-1,) + (1,) * (len(extent) - 1 - position))
    return factor_of


def routed_block(key, own, number, rows, number_of, top, reach, skew):
    ranking = jax.random.permutation(key, number_of)
    crowded, ordinary = shares(number_of, rows * top, reach, skew, True), shares(number_of, rows * top, reach, skew, False)
    places = jnp.arange(number_of)

    def named(sizes, rotation):
        used = int((sizes > 0).sum())
        fixed = max(1, used // 4)
        moved = fixed + (places - fixed + rotation * (used - fixed)) % max(1, number_of - fixed)
        return jnp.zeros((number_of,), jnp.int32).at[ranking[jnp.where(places < fixed, places, moved)]].set(jnp.asarray(sizes, jnp.int32))

    sizes = jnp.where(number % 4 == 0, named(crowded, number // 4), named(ordinary, number - number // 4 - 1))
    mixed = jax.random.permutation(jax.random.fold_in(own, 3), number_of)
    giver, receiver = mixed[0:number_of // 2 * 2:2], mixed[1:number_of // 2 * 2:2]
    room = jnp.minimum(sizes[giver] - 1, reach - sizes[receiver]) // 2
    room = jnp.where((giver == ranking[0]) | (receiver == ranking[0]) | (sizes[receiver] == 0), 0, jnp.maximum(room, 0))
    moved = jax.random.randint(jax.random.fold_in(own, 4), (number_of // 2,), 0, 1 << 20) % (room + 1)
    sizes = sizes.at[giver].add(-moved).at[receiver].add(moved)
    labels = jnp.searchsorted(jnp.cumsum(sizes), jnp.arange(rows * top), side="right").astype(jnp.int32)
    grid = labels.reshape(top, rows).T
    grid = grid[jax.random.permutation(jax.random.fold_in(own, 1), rows)]
    rotation = jax.random.randint(jax.random.fold_in(own, 2), (rows, 1), 0, top)
    return jnp.take_along_axis(grid, (jnp.arange(top)[None, :] + rotation) % top, axis=1)


def shares(number_of, total, reach, skew, full):
    portions = [(1 << 20) // math.isqrt(rank ** skew) + 1 for rank in range(1, number_of + 1)]
    largest = reach if full else min(reach, max(-(-total // number_of), total * portions[0] // sum(portions)))
    least = 1 if total - largest >= number_of - 1 else 0
    counts, spare = [largest] + [least] * (number_of - 1), total - largest - least * (number_of - 1)
    while spare > 0:
        candidates = [i for i in range(1, number_of) if counts[i] < largest] or [i for i in range(1, number_of) if counts[i] < reach]
        pool, budget = sum([portions[i] for i in candidates]), spare
        for i in candidates:
            extra = min(reach - counts[i], max(1, budget * portions[i] // pool), spare)
            counts[i] = counts[i] + extra
            spare = spare - extra
    return np.array(counts)


def gaussian(own_key, extent, deviation, most, cuts=(), kind=jnp.bfloat16):
    factor_of = block_scale(own_key, extent, cuts, -0.22, 0.18) if cuts else 1.0
    array = jax.random.normal(own_key, extent, jnp.float32) * deviation * factor_of
    return jnp.minimum(jnp.maximum(array, -most), most).astype(kind)


def setup_inputs(seed: int = 0) -> dict:
    keys = jax.random.split(jax.random.key(seed), 8)
    inputs = gaussian(keys[0], (SECTIONS, TOKENS, D), 1.0, 6.0, ((0, 4), (1, 8)))
    out_grads = gaussian(keys[1], (SECTIONS, TOKENS, D), 1.0, 6.0, ((0, 4), (1, 8)))
    expert_ids_keys = jax.random.split(jax.random.fold_in(keys[2], 1), SECTIONS * TOKENS // TOK_DEV)
    expert_ids_turns = jax.random.permutation(jax.random.fold_in(keys[2], 3), SECTIONS * TOKENS // TOK_DEV)
    expert_ids = jax.vmap(lambda own, number: routed_block(jax.random.fold_in(keys[2], 2), own, number, TOK_DEV, EXPERTS, TOPK, CAP, 2))(expert_ids_keys, expert_ids_turns).reshape((SECTIONS, TOKENS, TOPK))
    route_levels = set_ends(jax.random.randint(keys[3], (SECTIONS, TOKENS, TOPK), 8, 257), jax.random.fold_in(keys[3], 1), 8, 256).astype(jnp.int32)
    w_gate = gaussian(keys[4], (SECTIONS, EXPERTS, D, H), D ** -0.5, 0.1875, ((0, 4), (1, 8)))
    w_up = gaussian(keys[5], (SECTIONS, EXPERTS, D, H), D ** -0.5, 0.1875, ((0, 4), (1, 8)))
    w_down = gaussian(keys[6], (SECTIONS, EXPERTS, H, D), H ** -0.5, 0.3125, ((0, 4), (1, 8)))
    return {"inputs": inputs, "out_grads": out_grads, "expert_ids": expert_ids, "route_levels": route_levels, "w_gate": w_gate, "w_up": w_up, "w_down": w_down}


def flat_slots(expert_ids, experts_all, capacity):
    blocks = expert_ids.shape[0]
    flat_ids = expert_ids.reshape(blocks, -1).astype(jnp.int32)
    catalog = jnp.arange(experts_all, dtype=jnp.int32)
    onehot = (flat_ids[:, :, None] == catalog[None, None, :]).astype(jnp.int32)
    rank_table = (jnp.cumsum(onehot, axis=1) - 1).astype(jnp.int32)
    slot_of = jnp.sum(onehot * rank_table, axis=2).astype(jnp.int32)
    return (flat_ids * capacity + slot_of).astype(jnp.int32).reshape(expert_ids.shape)


def expert_backward(slot_inputs, slot_grads, slot_routes, w_gate, w_up, w_down):
    inputs_wide = slot_inputs.astype(jnp.float32)
    grads_wide = slot_grads.astype(jnp.float32)
    gate_wide = w_gate.astype(jnp.float32)
    up_wide = w_up.astype(jnp.float32)
    down_wide = w_down.astype(jnp.float32)
    gate_pre = jnp.einsum('esd,edh->esh', inputs_wide, gate_wide)
    up_pre = jnp.einsum('esd,edh->esh', inputs_wide, up_wide)
    sigmoid_gate = jax.nn.sigmoid(gate_pre)
    silu_gate = gate_pre * sigmoid_gate
    active = (silu_gate * up_pre).astype(jnp.bfloat16)
    active_wide = active.astype(jnp.float32)
    expert_out = jnp.einsum('esh,ehd->esd', active_wide, down_wide)
    route_part = jnp.sum(grads_wide * expert_out, axis=2).astype(jnp.bfloat16)
    weighted = (slot_routes.astype(jnp.float32)[:, :, None] * grads_wide).astype(jnp.bfloat16)
    weighted_wide = weighted.astype(jnp.float32)
    active_grad = jnp.einsum('esd,ehd->esh', weighted_wide, down_wide)
    gate_pre_grad = (active_grad * up_pre * sigmoid_gate * (1.0 + gate_pre * (1.0 - sigmoid_gate))).astype(jnp.bfloat16)
    up_pre_grad = (active_grad * silu_gate).astype(jnp.bfloat16)
    gate_grad_wide = gate_pre_grad.astype(jnp.float32)
    up_grad_wide = up_pre_grad.astype(jnp.float32)
    input_grad = (jnp.einsum('esh,edh->esd', gate_grad_wide, gate_wide)
                  + jnp.einsum('esh,edh->esd', up_grad_wide, up_wide)).astype(jnp.bfloat16)
    down_part = jnp.einsum('esh,esd->ehd', active_wide, weighted_wide).astype(jnp.bfloat16)
    gate_part = jnp.einsum('esd,esh->edh', inputs_wide, gate_grad_wide).astype(jnp.bfloat16)
    up_part = jnp.einsum('esd,esh->edh', inputs_wide, up_grad_wide).astype(jnp.bfloat16)
    return input_grad, route_part, gate_part, up_part, down_part


def section_backward(operands):
    inputs, out_grads, expert_ids, route_levels, w_gate, w_up, w_down = operands
    blocks = N_EXPERT
    flat_index = flat_slots(expert_ids.reshape(blocks, TOK_DEV, TOPK), EXPERTS, CAP)
    catalog = jnp.arange(EXPERTS * CAP, dtype=jnp.int32)
    select = (flat_index[..., None] == catalog).astype(jnp.float32).reshape(blocks, TOK_DEV, TOPK, EXPERTS, CAP)
    placing = jnp.sum(select, axis=2)
    route_values = (route_levels.astype(jnp.float32) / 256.0).reshape(blocks, TOK_DEV, TOPK)
    inputs_wide = inputs.astype(jnp.float32).reshape(blocks, TOK_DEV, D)
    grads_wide = out_grads.astype(jnp.float32).reshape(blocks, TOK_DEV, D)
    slot_inputs = jnp.einsum('btec,btd->ebcd', placing, inputs_wide).reshape(EXPERTS, blocks * CAP, D).astype(jnp.bfloat16)
    slot_grads = jnp.einsum('btec,btd->ebcd', placing, grads_wide).reshape(EXPERTS, blocks * CAP, D).astype(jnp.bfloat16)
    slot_routes = jnp.einsum('btkec,btk->ebc', select, route_values).reshape(EXPERTS, blocks * CAP).astype(jnp.bfloat16)
    input_grad, route_part, gate_part, up_part, down_part = expert_backward(slot_inputs, slot_grads, slot_routes, w_gate, w_up, w_down)
    back_inputs = input_grad.astype(jnp.float32).reshape(EXPERTS, blocks, CAP, D)
    token_grad = jnp.einsum('btec,ebcd->btd', placing, back_inputs).reshape(TOKENS, D).astype(jnp.bfloat16)
    back_routes = route_part.astype(jnp.float32).reshape(EXPERTS, blocks, CAP)
    token_route = jnp.einsum('btkec,ebc->btk', select, back_routes).reshape(TOKENS, TOPK).astype(jnp.bfloat16)
    return token_grad, token_route, gate_part, up_part, down_part


def reference(inputs, out_grads, expert_ids, route_levels, w_gate, w_up, w_down):
    token_grad, token_route, gate_part, up_part, down_part = lax.map(
        section_backward, (inputs, out_grads, expert_ids, route_levels, w_gate, w_up, w_down))
    upstream = jnp.concatenate([token_grad[1:], jnp.zeros_like(token_grad[:1])], axis=0)
    return upstream, token_route, gate_part, up_part, down_part
```

```python
import functools
import math

import jax
import jax.numpy as jnp
from jax import lax
from jax.experimental import pallas as pl
from jax.experimental.pallas import tpu as pltpu
from jax.sharding import PartitionSpec as P

MESH = pl.DeviceIdType.MESH
INFO = 128


def kernel(
    lines, rows, sections,
    in_ref, grad_ref, route_ref, wg_ref, wu_ref, wd_ref,
    up_ref, own_route_ref, gate_ref, up_out_ref, down_ref,
    packed, w_in, w_down, hidden_grads, scaled_all, x_out, x_in, z_out, z_in, token,
    load_sem, weight_sem, store_sem,
    az_send, ax_send, a_recv, rx_send, rx_recv, rz_send, rz_recv, y_send, y_recv,
):
    blocks = lines * rows
    tok, width = in_ref.shape
    local, _, hidden = wg_ref.shape
    me = lax.axis_index("expert")
    section = lax.axis_index("section")
    z, x = me // rows, lax.rem(me, rows)

    def at(dz, dx):
        return lax.rem(z + dz, lines) * rows + lax.rem(x + dx, rows)

    loads = [
        pltpu.make_async_copy(in_ref, packed.at[me, :, pl.ds(0, width)], load_sem.at[0]),
        pltpu.make_async_copy(grad_ref, packed.at[me, :, pl.ds(width, width)], load_sem.at[1]),
        pltpu.make_async_copy(route_ref, packed.at[me, :, pl.ds(2 * width, INFO)], load_sem.at[2]),
    ]
    weights = []
    for e in range(local):
        weights.append((wg_ref.at[e], w_in.at[:, pl.ds(2 * e * hidden, hidden)]))
        weights.append((wu_ref.at[e], w_in.at[:, pl.ds((2 * e + 1) * hidden, hidden)]))
        weights.append((wd_ref.at[e], w_down.at[pl.ds(e * hidden, hidden), :]))
    weights = [pltpu.make_async_copy(a, b, weight_sem.at[i]) for i, (a, b) in enumerate(weights)]
    for copy in loads + weights:
        copy.start()

    barrier = pltpu.get_barrier_semaphore()
    for dz in range(1, lines):
        pl.semaphore_signal(barrier, inc=1, device_id={"expert": at(dz, 0)}, device_id_type=MESH)
    for dx in range(1, rows):
        pl.semaphore_signal(barrier, inc=1, device_id={"expert": at(0, dx)}, device_id_type=MESH)
    before = lax.rem(section + sections - 1, sections)
    after = lax.rem(section + 1, sections)
    for other in (before, after):
        pl.semaphore_signal(barrier, inc=1, device_id={"section": other}, device_id_type=MESH)
    pl.semaphore_wait(barrier, lines + rows)

    def gather_z(dz):
        return pltpu.make_async_remote_copy(
            src_ref=packed.at[me], dst_ref=packed.at[me],
            send_sem=az_send.at[dz], recv_sem=a_recv.at[me],
            device_id={"expert": at(dz, 0)}, device_id_type=MESH,
        )

    def gather_x(dz, dx):
        block = at(dz, 0)
        return pltpu.make_async_remote_copy(
            src_ref=packed.at[block], dst_ref=packed.at[block],
            send_sem=ax_send.at[dz, dx], recv_sem=a_recv.at[block],
            device_id={"expert": at(0, dx)}, device_id_type=MESH,
        )

    def arrived(block):
        pltpu.make_async_remote_copy(
            src_ref=packed.at[block], dst_ref=packed.at[block],
            send_sem=az_send.at[0], recv_sem=a_recv.at[block],
            device_id={"expert": at(1, 0)}, device_id_type=MESH,
        ).wait_recv()

    def reduce_x(dz, dx):
        line = lax.rem(z + dz, lines)
        return pltpu.make_async_remote_copy(
            src_ref=x_out.at[line, dx - 1], dst_ref=x_in.at[line, dx - 1],
            send_sem=rx_send.at[line, dx - 1], recv_sem=rx_recv.at[line, dx - 1],
            device_id={"expert": at(0, dx)}, device_id_type=MESH,
        )

    def reduce_z(dz):
        line = lax.rem(z + dz, lines)
        return pltpu.make_async_remote_copy(
            src_ref=z_out.at[line], dst_ref=z_in.at[dz],
            send_sem=rz_send.at[dz], recv_sem=rz_recv.at[dz],
            device_id={"expert": at(dz, 0)}, device_id_type=MESH,
        )

    for copy in loads:
        copy.wait()
    for dx in range(1, rows):
        gather_x(0, dx).start()
    for dz in range(1, lines):
        gather_z(dz).start()
    for copy in weights:
        copy.wait()

    catalog = lax.broadcasted_iota(jnp.int32, (tok, INFO), 1)
    first = me * local
    last_dims = (((1,), (1,)), ((), ()))

    def compute(block):
        route_all = packed[block, :, pl.ds(2 * width, INFO)].astype(jnp.float32)
        pre = jnp.dot(packed[block, :, pl.ds(0, width)], w_in[...], preferred_element_type=jnp.float32)
        back_all = lax.dot_general(
            packed[block, :, pl.ds(width, width)], w_down[...], last_dims,
            preferred_element_type=jnp.float32,
        )
        route_out = jnp.zeros((tok, INFO), jnp.float32)
        for e in range(local):
            mine = catalog == first + e
            route = jnp.sum(jnp.where(mine, route_all, 0.0), axis=1, keepdims=True)
            gate = pre[:, 2 * e * hidden : (2 * e + 1) * hidden]
            up = pre[:, (2 * e + 1) * hidden : (2 * e + 2) * hidden]
            back = back_all[:, e * hidden : (e + 1) * hidden]
            sig = jax.nn.sigmoid(gate)
            silu = gate * sig
            active = silu * up
            route_grad = jnp.sum(active * back, axis=1, keepdims=True)
            route_out = route_out + jnp.where(mine, route_grad, 0.0)
            back = back * route
            hidden_grads[block, :, pl.ds(2 * e * hidden, hidden)] = (
                back * up * sig * (1.0 + gate * (1.0 - sig))
            ).astype(jnp.bfloat16)
            hidden_grads[block, :, pl.ds((2 * e + 1) * hidden, hidden)] = (back * silu).astype(jnp.bfloat16)
            scaled_all[block, :, pl.ds(e * hidden, hidden)] = (active * route).astype(jnp.bfloat16)
        total = lax.dot_general(
            hidden_grads[block], w_in[...], last_dims, preferred_element_type=jnp.float32
        )
        return total.astype(jnp.bfloat16), route_out.astype(jnp.bfloat16)

    def send_line(dz):
        line = lax.rem(z + dz, lines)
        for dx in range(1, rows):
            reduce_x(dz, dx).wait_recv()
        value = z_out[line].astype(jnp.float32)
        for dx in range(1, rows):
            value = value + x_in[line, dx - 1].astype(jnp.float32)
        z_out[line] = value.astype(jnp.bfloat16)

    def step(j, carry):
        dz, dx = j // rows, lax.rem(j, rows)
        block = at(dz, dx)
        line = lax.rem(z + dz, lines)

        @pl.when(j > 0)
        def _():
            arrived(block)

        @pl.when((dx == 0) & (dz > 0))
        def _():
            for other in range(1, rows):
                gather_x(dz, other).start()

        total, route_out = compute(block)

        @pl.when(dx == 0)
        def _():
            z_out[line, :, pl.ds(0, width)] = total
            z_out[line, :, pl.ds(width, INFO)] = route_out

        @pl.when(dx > 0)
        def _():
            x_out[line, dx - 1, :, pl.ds(0, width)] = total
            x_out[line, dx - 1, :, pl.ds(width, INFO)] = route_out
            reduce_x(dz, dx).start()

        @pl.when((dx == 0) & (dz > 1))
        def _():
            send_line(dz - 1)
            reduce_z(dz - 1).start()

        return carry

    lax.fori_loop(0, blocks, step, 0)
    send_line(lines - 1)
    reduce_z(lines - 1).start()

    first_dims = (((0,), (0,)), ((), ()))
    all_rows = blocks * tok
    tile = 256 if width % 256 == 0 and (local * hidden) % 256 == 0 else 128

    @pl.loop(0, width // tile)
    def _(c):
        at_c = pl.ds(pl.multiple_of(c * tile, tile), tile)
        left = packed[:, :, at_c].reshape(all_rows, tile)
        right = hidden_grads[...].reshape(all_rows, 2 * local * hidden)
        w_in[at_c, :] = lax.dot_general(
            left, right, first_dims, preferred_element_type=jnp.float32
        ).astype(jnp.bfloat16)

    stores = []
    for e in range(local):
        stores.append((w_in.at[:, pl.ds(2 * e * hidden, hidden)], gate_ref.at[e]))
        stores.append((w_in.at[:, pl.ds((2 * e + 1) * hidden, hidden)], up_out_ref.at[e]))
    for e in range(local):
        stores.append((w_down.at[pl.ds(e * hidden, hidden), :], down_ref.at[e]))
    stores = [pltpu.make_async_copy(a, b, store_sem.at[i]) for i, (a, b) in enumerate(stores)]
    for copy in stores[: 2 * local]:
        copy.start()

    send_line(0)
    value = z_out[z].astype(jnp.float32)
    for dz in range(1, lines):
        reduce_z(dz).wait_recv()
        value = value + z_in[dz].astype(jnp.float32)
    token[...] = value[:, :width].astype(jnp.bfloat16)
    own_route_ref[...] = value[:, width:].astype(jnp.bfloat16)

    hop = pltpu.make_async_remote_copy(
        src_ref=token, dst_ref=up_ref, send_sem=y_send, recv_sem=y_recv,
        device_id={"section": before}, device_id_type=MESH,
    )

    @pl.when(section > 0)
    def _():
        hop.start()

    @pl.when(section == sections - 1)
    def _():
        up_ref[...] = jnp.zeros_like(up_ref)

    @pl.loop(0, local * hidden // tile)
    def _(c):
        at_c = pl.ds(pl.multiple_of(c * tile, tile), tile)
        left = scaled_all[:, :, at_c].reshape(all_rows, tile)
        right = packed[:, :, pl.ds(width, width)].reshape(all_rows, width)
        w_down[at_c, :] = lax.dot_general(
            left, right, first_dims, preferred_element_type=jnp.float32
        ).astype(jnp.bfloat16)

    for copy in stores[2 * local :]:
        copy.start()
    for dz in range(1, lines):
        gather_z(dz).wait_send()
        reduce_z(dz).wait_send()
    for dz in range(lines):
        for dx in range(1, rows):
            gather_x(dz, dx).wait_send()
            reduce_x(dz, dx).wait_send()

    @pl.when(section > 0)
    def _():
        hop.wait_send()

    @pl.when(section < sections - 1)
    def _():
        hop.wait_recv()

    for copy in stores:
        copy.wait()


def body(rows, inputs, out_grads, expert_ids, route_levels, w_gate, w_up, w_down):
    tok, width = inputs.shape[1:]
    local, _, hidden = w_gate.shape[1:]
    blocks = lax.axis_size("expert")
    sections = lax.axis_size("section")
    lines = blocks // rows
    catalog = jnp.arange(INFO, dtype=jnp.int32)
    chosen = expert_ids[0][:, :, None] == catalog
    levels = jnp.sum(jnp.where(chosen, route_levels[0][:, :, None], 0), axis=1)
    routes = (levels.astype(jnp.float32) / 256.0).astype(jnp.bfloat16)
    bf16 = jnp.bfloat16
    anywhere = pl.BlockSpec(memory_space=pl.ANY)
    inside = pl.BlockSpec(memory_space=pltpu.VMEM)
    dma = pltpu.SemaphoreType.DMA
    side = max(rows - 1, 1)
    upstream, own_routes, gates, ups, downs = pl.pallas_call(
        functools.partial(kernel, lines, rows, sections),
        out_shape=(
            jax.ShapeDtypeStruct((tok, width), bf16),
            jax.ShapeDtypeStruct((tok, INFO), bf16),
            jax.ShapeDtypeStruct(w_gate.shape[1:], bf16),
            jax.ShapeDtypeStruct(w_up.shape[1:], bf16),
            jax.ShapeDtypeStruct(w_down.shape[1:], bf16),
        ),
        in_specs=[anywhere] * 6,
        out_specs=(inside, inside, anywhere, anywhere, anywhere),
        scratch_shapes=[
            pltpu.VMEM((blocks, tok, 2 * width + INFO), bf16),
            pltpu.VMEM((width, 2 * local * hidden), bf16),
            pltpu.VMEM((local * hidden, width), bf16),
            pltpu.VMEM((blocks, tok, 2 * local * hidden), bf16),
            pltpu.VMEM((blocks, tok, local * hidden), bf16),
            pltpu.VMEM((lines, side, tok, width + INFO), bf16),
            pltpu.VMEM((lines, side, tok, width + INFO), bf16),
            pltpu.VMEM((lines, tok, width + INFO), bf16),
            pltpu.VMEM((lines, tok, width + INFO), bf16),
            pltpu.VMEM((tok, width), bf16),
            dma((3,)),
            dma((3 * local,)),
            dma((3 * local,)),
            dma((lines,)),
            dma((lines, rows)),
            dma((blocks,)),
            dma((lines, side)),
            dma((lines, side)),
            dma((lines,)),
            dma((lines,)),
            dma,
            dma,
        ],
        compiler_params=pltpu.CompilerParams(
            collective_id=0, has_side_effects=True, vmem_limit_bytes=66_000_000
        ),
    )(inputs[0], out_grads[0], routes, w_gate[0], w_up[0], w_down[0])
    token_route = jnp.sum(
        jnp.where(chosen, own_routes[:, None, :].astype(jnp.float32), 0.0), axis=2
    ).astype(bf16)
    return (upstream[None], token_route[None], gates[None], ups[None], downs[None])


def solution(mesh):
    blocks = mesh.shape["expert"]
    rows = math.isqrt(max(blocks // 2, 1))
    while blocks % rows:
        rows -= 1
    in_specs = (
        P("section", "expert", None),
        P("section", "expert", None),
        P("section", "expert", None),
        P("section", "expert", None),
        P("section", "expert", None, None),
        P("section", "expert", None, None),
        P("section", "expert", None, None),
    )
    out_specs = (
        P("section", "expert", None),
        P("section", "expert", None),
        P("section", "expert", None, None),
        P("section", "expert", None, None),
        P("section", "expert", None, None),
    )
    return jax.shard_map(
        functools.partial(body, rows), mesh=mesh, in_specs=in_specs, out_specs=out_specs, check_vma=False
    )
```

```python
import functools
import math

import jax
import jax.numpy as jnp
from jax import lax
from jax.experimental import pallas as pl
from jax.experimental.pallas import tpu as pltpu
from jax.sharding import PartitionSpec as P

MESH = pl.DeviceIdType.MESH
INFO = 128


def kernel(
    lines, rows, sections,
    in_ref, grad_ref, route_ref, wg_ref, wu_ref, wd_ref,
    up_ref, own_route_ref, gate_ref, up_out_ref, down_ref,
    packed, w_in, w_down, hidden_grads, scaled_all, x_out, x_in, z_out, z_in, token,
    load_sem, weight_sem, store_sem,
    az_send, ax_send, a_recv, rx_send, rx_recv, rz_send, rz_recv, y_send, y_recv,
):
    blocks = lines * rows
    tok, width = in_ref.shape
    local, _, hidden = wg_ref.shape
    me = lax.axis_index("expert")
    section = lax.axis_index("section")
    z, x = me // rows, lax.rem(me, rows)

    def paired(d):
        if lines & (lines - 1):
            return lax.rem(z + d, lines)
        bits = lines.bit_length() - 1
        return sum(((z // 2**i + d // 2**i) % 2) * 2**i for i in range(bits))

    def at(dz, dx):
        return paired(dz) * rows + lax.rem(x + dx, rows)

    loads = [
        pltpu.make_async_copy(in_ref, packed.at[me, :, pl.ds(0, width)], load_sem.at[0]),
        pltpu.make_async_copy(grad_ref, packed.at[me, :, pl.ds(width, width)], load_sem.at[1]),
        pltpu.make_async_copy(route_ref, packed.at[me, :, pl.ds(2 * width, INFO)], load_sem.at[2]),
    ]
    weights = []
    for e in range(local):
        weights.append((wg_ref.at[e], w_in.at[:, pl.ds(2 * e * hidden, hidden)]))
        weights.append((wu_ref.at[e], w_in.at[:, pl.ds((2 * e + 1) * hidden, hidden)]))
        weights.append((wd_ref.at[e], w_down.at[pl.ds(e * hidden, hidden), :]))
    weights = [pltpu.make_async_copy(a, b, weight_sem.at[i]) for i, (a, b) in enumerate(weights)]
    for copy in loads + weights:
        copy.start()

    barrier = pltpu.get_barrier_semaphore()
    for dz in range(1, lines):
        pl.semaphore_signal(barrier, inc=1, device_id={"expert": at(dz, 0)}, device_id_type=MESH)
    for dx in range(1, rows):
        pl.semaphore_signal(barrier, inc=1, device_id={"expert": at(0, dx)}, device_id_type=MESH)
    before = lax.rem(section + sections - 1, sections)
    after = lax.rem(section + 1, sections)
    for other in (before, after):
        pl.semaphore_signal(barrier, inc=1, device_id={"section": other}, device_id_type=MESH)
    pl.semaphore_wait(barrier, lines + rows)

    def gather_z(dz):
        return pltpu.make_async_remote_copy(
            src_ref=packed.at[me], dst_ref=packed.at[me],
            send_sem=az_send.at[dz], recv_sem=a_recv.at[me],
            device_id={"expert": at(dz, 0)}, device_id_type=MESH,
        )

    def gather_x(dz, dx):
        block = at(dz, 0)
        return pltpu.make_async_remote_copy(
            src_ref=packed.at[block], dst_ref=packed.at[block],
            send_sem=ax_send.at[dz, dx], recv_sem=a_recv.at[block],
            device_id={"expert": at(0, dx)}, device_id_type=MESH,
        )

    def arrived(block):
        pltpu.make_async_remote_copy(
            src_ref=packed.at[block], dst_ref=packed.at[block],
            send_sem=az_send.at[0], recv_sem=a_recv.at[block],
            device_id={"expert": at(1, 0)}, device_id_type=MESH,
        ).wait_recv()

    def reduce_x(dz, dx):
        line = paired(dz)
        return pltpu.make_async_remote_copy(
            src_ref=x_out.at[line, dx - 1], dst_ref=x_in.at[line, dx - 1],
            send_sem=rx_send.at[line, dx - 1], recv_sem=rx_recv.at[line, dx - 1],
            device_id={"expert": at(0, dx)}, device_id_type=MESH,
        )

    def reduce_z(dz):
        line = paired(dz)
        return pltpu.make_async_remote_copy(
            src_ref=z_out.at[line], dst_ref=z_in.at[dz],
            send_sem=rz_send.at[dz], recv_sem=rz_recv.at[dz],
            device_id={"expert": at(dz, 0)}, device_id_type=MESH,
        )

    for copy in loads:
        copy.wait()
    for dx in range(1, rows):
        gather_x(0, dx).start()
    for dz in range(1, lines):
        gather_z(dz).start()
    for copy in weights:
        copy.wait()

    catalog = lax.broadcasted_iota(jnp.int32, (tok, INFO), 1)
    first = me * local
    last_dims = (((1,), (1,)), ((), ()))

    def compute(block):
        route_all = packed[block, :, pl.ds(2 * width, INFO)].astype(jnp.float32)
        pre = jnp.dot(packed[block, :, pl.ds(0, width)], w_in[...], preferred_element_type=jnp.float32)
        back_all = lax.dot_general(
            packed[block, :, pl.ds(width, width)], w_down[...], last_dims,
            preferred_element_type=jnp.float32,
        )
        route_out = jnp.zeros((tok, INFO), jnp.float32)
        for e in range(local):
            mine = catalog == first + e
            route = jnp.sum(jnp.where(mine, route_all, 0.0), axis=1, keepdims=True)
            gate = pre[:, 2 * e * hidden : (2 * e + 1) * hidden]
            up = pre[:, (2 * e + 1) * hidden : (2 * e + 2) * hidden]
            back = back_all[:, e * hidden : (e + 1) * hidden]
            sig = jax.nn.sigmoid(gate)
            silu = gate * sig
            active = silu * up
            route_grad = jnp.sum(active * back, axis=1, keepdims=True)
            route_out = route_out + jnp.where(mine, route_grad, 0.0)
            back = back * route
            hidden_grads[block, :, pl.ds(2 * e * hidden, hidden)] = (
                back * up * sig * (1.0 + gate * (1.0 - sig))
            ).astype(jnp.bfloat16)
            hidden_grads[block, :, pl.ds((2 * e + 1) * hidden, hidden)] = (back * silu).astype(jnp.bfloat16)
            scaled_all[block, :, pl.ds(e * hidden, hidden)] = (active * route).astype(jnp.bfloat16)
        total = lax.dot_general(
            hidden_grads[block], w_in[...], last_dims, preferred_element_type=jnp.float32
        )
        return total.astype(jnp.bfloat16), route_out.astype(jnp.bfloat16)

    def send_line(dz):
        line = paired(dz)
        for dx in range(1, rows):
            reduce_x(dz, dx).wait_recv()
        value = z_out[line].astype(jnp.float32)
        for dx in range(1, rows):
            value = value + x_in[line, dx - 1].astype(jnp.float32)
        z_out[line] = value.astype(jnp.bfloat16)

    def step(j, carry):
        dz, dx = j // rows, lax.rem(j, rows)
        block = at(dz, dx)
        line = paired(dz)

        @pl.when(j > 0)
        def _():
            arrived(block)

        @pl.when((dx == 0) & (dz > 0))
        def _():
            for other in range(1, rows):
                gather_x(dz, other).start()

        total, route_out = compute(block)

        @pl.when(dx == 0)
        def _():
            z_out[line, :, pl.ds(0, width)] = total
            z_out[line, :, pl.ds(width, INFO)] = route_out

        @pl.when(dx > 0)
        def _():
            x_out[line, dx - 1, :, pl.ds(0, width)] = total
            x_out[line, dx - 1, :, pl.ds(width, INFO)] = route_out
            reduce_x(dz, dx).start()

        @pl.when((dx == 0) & (dz > 1))
        def _():
            send_line(dz - 1)
            reduce_z(dz - 1).start()

        return carry

    lax.fori_loop(0, blocks, step, 0)
    send_line(lines - 1)
    reduce_z(lines - 1).start()

    first_dims = (((0,), (0,)), ((), ()))
    all_rows = blocks * tok
    tile = 256 if width % 256 == 0 and (local * hidden) % 256 == 0 else 128

    @pl.loop(0, width // tile)
    def _(c):
        at_c = pl.ds(pl.multiple_of(c * tile, tile), tile)
        left = packed[:, :, at_c].reshape(all_rows, tile)
        right = hidden_grads[...].reshape(all_rows, 2 * local * hidden)
        w_in[at_c, :] = lax.dot_general(
            left, right, first_dims, preferred_element_type=jnp.float32
        ).astype(jnp.bfloat16)

    stores = []
    for e in range(local):
        stores.append((w_in.at[:, pl.ds(2 * e * hidden, hidden)], gate_ref.at[e]))
        stores.append((w_in.at[:, pl.ds((2 * e + 1) * hidden, hidden)], up_out_ref.at[e]))
    for e in range(local):
        stores.append((w_down.at[pl.ds(e * hidden, hidden), :], down_ref.at[e]))
    stores = [pltpu.make_async_copy(a, b, store_sem.at[i]) for i, (a, b) in enumerate(stores)]
    for copy in stores[: 2 * local]:
        copy.start()

    send_line(0)
    value = z_out[z].astype(jnp.float32)
    for dz in range(1, lines):
        reduce_z(dz).wait_recv()
        value = value + z_in[dz].astype(jnp.float32)
    token[...] = value[:, :width].astype(jnp.bfloat16)
    own_route_ref[...] = value[:, width:].astype(jnp.bfloat16)

    hop = pltpu.make_async_remote_copy(
        src_ref=token, dst_ref=up_ref, send_sem=y_send, recv_sem=y_recv,
        device_id={"section": before}, device_id_type=MESH,
    )

    @pl.when(section > 0)
    def _():
        hop.start()

    @pl.when(section == sections - 1)
    def _():
        up_ref[...] = jnp.zeros_like(up_ref)

    @pl.loop(0, local * hidden // tile)
    def _(c):
        at_c = pl.ds(pl.multiple_of(c * tile, tile), tile)
        left = scaled_all[:, :, at_c].reshape(all_rows, tile)
        right = packed[:, :, pl.ds(width, width)].reshape(all_rows, width)
        w_down[at_c, :] = lax.dot_general(
            left, right, first_dims, preferred_element_type=jnp.float32
        ).astype(jnp.bfloat16)

    for copy in stores[2 * local :]:
        copy.start()
    for dz in range(1, lines):
        gather_z(dz).wait_send()
        reduce_z(dz).wait_send()
    for dz in range(lines):
        for dx in range(1, rows):
            gather_x(dz, dx).wait_send()
            reduce_x(dz, dx).wait_send()

    @pl.when(section > 0)
    def _():
        hop.wait_send()

    @pl.when(section < sections - 1)
    def _():
        hop.wait_recv()

    for copy in stores:
        copy.wait()


def body(rows, inputs, out_grads, expert_ids, route_levels, w_gate, w_up, w_down):
    tok, width = inputs.shape[1:]
    local, _, hidden = w_gate.shape[1:]
    blocks = lax.axis_size("expert")
    sections = lax.axis_size("section")
    lines = blocks // rows
    catalog = jnp.arange(INFO, dtype=jnp.int32)
    chosen = expert_ids[0][:, :, None] == catalog
    levels = jnp.sum(jnp.where(chosen, route_levels[0][:, :, None], 0), axis=1)
    routes = (levels.astype(jnp.float32) / 256.0).astype(jnp.bfloat16)
    bf16 = jnp.bfloat16
    anywhere = pl.BlockSpec(memory_space=pl.ANY)
    inside = pl.BlockSpec(memory_space=pltpu.VMEM)
    dma = pltpu.SemaphoreType.DMA
    side = max(rows - 1, 1)
    upstream, own_routes, gates, ups, downs = pl.pallas_call(
        functools.partial(kernel, lines, rows, sections),
        out_shape=(
            jax.ShapeDtypeStruct((tok, width), bf16),
            jax.ShapeDtypeStruct((tok, INFO), bf16),
            jax.ShapeDtypeStruct(w_gate.shape[1:], bf16),
            jax.ShapeDtypeStruct(w_up.shape[1:], bf16),
            jax.ShapeDtypeStruct(w_down.shape[1:], bf16),
        ),
        in_specs=[anywhere] * 6,
        out_specs=(inside, inside, anywhere, anywhere, anywhere),
        scratch_shapes=[
            pltpu.VMEM((blocks, tok, 2 * width + INFO), bf16),
            pltpu.VMEM((width, 2 * local * hidden), bf16),
            pltpu.VMEM((local * hidden, width), bf16),
            pltpu.VMEM((blocks, tok, 2 * local * hidden), bf16),
            pltpu.VMEM((blocks, tok, local * hidden), bf16),
            pltpu.VMEM((lines, side, tok, width + INFO), bf16),
            pltpu.VMEM((lines, side, tok, width + INFO), bf16),
            pltpu.VMEM((lines, tok, width + INFO), bf16),
            pltpu.VMEM((lines, tok, width + INFO), bf16),
            pltpu.VMEM((tok, width), bf16),
            dma((3,)),
            dma((3 * local,)),
            dma((3 * local,)),
            dma((lines,)),
            dma((lines, rows)),
            dma((blocks,)),
            dma((lines, side)),
            dma((lines, side)),
            dma((lines,)),
            dma((lines,)),
            dma,
            dma,
        ],
        compiler_params=pltpu.CompilerParams(
            collective_id=0, has_side_effects=True, vmem_limit_bytes=66_000_000
        ),
    )(inputs[0], out_grads[0], routes, w_gate[0], w_up[0], w_down[0])
    token_route = jnp.sum(
        jnp.where(chosen, own_routes[:, None, :].astype(jnp.float32), 0.0), axis=2
    ).astype(bf16)
    return (upstream[None], token_route[None], gates[None], ups[None], downs[None])


def solution(mesh):
    blocks = mesh.shape["expert"]
    rows = math.isqrt(max(blocks // 2, 1))
    while blocks % rows:
        rows -= 1
    in_specs = (
        P("section", "expert", None),
        P("section", "expert", None),
        P("section", "expert", None),
        P("section", "expert", None),
        P("section", "expert", None, None),
        P("section", "expert", None, None),
        P("section", "expert", None, None),
    )
    out_specs = (
        P("section", "expert", None),
        P("section", "expert", None),
        P("section", "expert", None, None),
        P("section", "expert", None, None),
        P("section", "expert", None, None),
    )
    return jax.shard_map(
        functools.partial(body, rows), mesh=mesh, in_specs=in_specs, out_specs=out_specs, check_vma=False
    )
```
